32 devices in a mesh: gy: 8 (over z, x), gx: 4 (over y, core).
Axes of the slice: x: 2, y: 2, z: 4, core: 2. Of those that a mesh axis runs over, the one named last changes fastest.
Arguments:
- tall_factor: bfloat16 [8192, 2048], P('gy', 'gx'), may hold values from -6 to 6
- wide_factor: bfloat16 [2048, 4096], P('gy', 'gx'), may hold values from -0.125 to 0.125
- target: float32 [8192, 4096], P('gy', 'gx'), may hold values from -6 to 6
Outputs:
- product_sum: float32 [8192, 4096], P('gy', 'gx')
The draws below stay inside these ranges and needn't reach their ends.
All inputs are finite; a program needn't handle non-finite values.
Results may differ from the reference program's by a relative error of at most 0.0003.
Values may be sent and summed in bfloat16 or wider, within the bound.
A program may use at most 128 MiB of HBM per device.

```python
import jax
import jax.numpy as jnp
from jax import lax

ROWS = 8192
COLS = 4096
INNER = 2048


def level_of(rng, extent, shards, least, top_value):
    def one(position, shards_of):
        heights = jax.random.uniform(jax.random.fold_in(jax.random.fold_in(rng, 6), position), (shards_of,), jnp.float32, least / len(shards), top_value / len(shards))
        return jnp.repeat(jnp.exp(heights), extent[position] // shards_of).reshape((-1,) + (1,) * (len(extent) - position - 1))

    gain = one(*shards[0])
    for cut in shards[1:]:
        gain = gain * one(*cut)
    return gain


def scatter_about(stream_key, extent, scale, most, split=(), held_as=jnp.bfloat16):
    entries = scale * jax.random.normal(stream_key, extent, jnp.float32)
    if split:
        entries = entries * level_of(stream_key, extent, split, -0.22, 0.18)
    return jnp.clip(entries, -most, most).astype(held_as)


def setup_inputs(seed: int = 0) -> dict:
    key_list = jax.random.split(jax.random.key(seed), 4)
    return {
        "tall_factor": scatter_about(key_list[0], (ROWS, INNER), 1.0, 6.0, ((0, 8), (1, 4))),
        "wide_factor": scatter_about(key_list[1], (INNER, COLS), INNER ** -0.5, 0.125, ((0, 8), (1, 4))),
        "target": scatter_about(key_list[2], (ROWS, COLS), 1.0, 6.0, ((0, 8), (1, 4)), jnp.float32),
    }


def reference(tall_factor, wide_factor, target):
    product_sum = target - jnp.dot(tall_factor, wide_factor, preferred_element_type=jnp.float32)
    row_power = lax.optimization_barrier(jnp.sum(product_sum * product_sum, axis=1))
    product_sum = product_sum * lax.rsqrt(row_power / COLS + 1e-06)[:, None]
    return product_sum
```

```python
import functools

import jax
import jax.numpy as jnp
from jax import lax
from jax.experimental import pallas as pl
from jax.experimental.pallas import tpu as pltpu
from jax.sharding import PartitionSpec as P

MESH = pl.DeviceIdType.MESH
LANES = 128
HALVES = 2


def kernel(
    n, m, a_hbm, b_hbm, t_hbm, o_hbm, p_out,
    a_buf, b_buf, acc, p_buf,
    a_recv, b_recv, p_recv, a_send, b_send, p_send, l_sem,
):
    gy, gx = lax.axis_index("gy"), lax.axis_index("gx")
    depth, cols = b_hbm.shape
    rows = a_hbm.shape[0]
    per = a_hbm.shape[1] // depth
    wide = cols // HALVES
    line = n // 2
    z, x = gy // 2, gy % 2
    has_left, has_right = z > 0, z < line - 1
    left, right, across = gy - 2, gy + 2, z * 2 + 1 - x
    mate = (gx // 2) * 2 + 1 - gx % 2
    others = [lax.rem(gx + j, m) for j in range(1, m)]
    far = [lax.rem(gx + 2 * j, m) for j in range(1, m // 2)]

    loads_b = pltpu.make_async_copy(b_hbm, b_buf.at[gy], l_sem.at[0])
    loads_b.start()
    loads_a = []
    for i in range(per):
        c = pltpu.make_async_copy(
            a_hbm.at[:, pl.ds(i * depth, depth)], a_buf.at[gx * per + i], l_sem.at[2 + i]
        )
        c.start()
        loads_a.append(c)
    load_t = pltpu.make_async_copy(t_hbm, acc, l_sem.at[1])
    load_t.start()

    barrier = pltpu.get_barrier_semaphore()
    for g in others:
        pl.semaphore_signal(barrier, 1, device_id=(gy, g), device_id_type=MESH)
    pl.semaphore_signal(barrier, 1, device_id=(across, gx), device_id_type=MESH)

    @pl.when(has_left)
    def _():
        pl.semaphore_signal(barrier, 1, device_id=(left, gx), device_id_type=MESH)

    @pl.when(has_right)
    def _():
        pl.semaphore_signal(barrier, 1, device_id=(right, gx), device_id_type=MESH)

    pl.semaphore_wait(
        barrier, m + has_left.astype(jnp.int32) + has_right.astype(jnp.int32)
    )

    sends = []

    def when(cond, f):
        if cond is None:
            f()
        else:
            pl.when(cond)(f)

    def both(p, q):
        return q if p is None else jnp.logical_and(p, q)

    def b_copy(way, to, k, h):
        part = b_buf.at[k, :, pl.ds(h * wide, wide)]
        return pltpu.make_async_remote_copy(
            part, part, b_send.at[way, k, h], b_recv.at[k, h],
            device_id=(to, gx), device_id_type=MESH,
        )

    def send_b(cond, way, to, k, h):
        make = functools.partial(b_copy, way, to, k, h)
        when(cond, lambda: make().start())
        sends.append((cond, make))

    def a_copy(way, to, k):
        return pltpu.make_async_remote_copy(
            a_buf.at[k], a_buf.at[k], a_send.at[way, k], a_recv.at[k],
            device_id=(gy, to), device_id_type=MESH,
        )

    def send_a(way, to, k):
        make = functools.partial(a_copy, way, to, k)
        make().start()
        sends.append((None, make))

    def wait_b(k, h):
        b_copy(0, gy, k, h).wait_recv()

    def wait_a(k):
        a_copy(0, gx, k).wait_recv()

    tile = min(rows, 512)

    def multiply(k, h):
        at = pl.multiple_of(h * wide, wide)

        @pl.loop(0, rows // tile)
        def _(i):
            r = pl.ds(pl.multiple_of(i * tile, tile), tile)
            acc[r, pl.ds(at, wide)] -= jnp.dot(
                a_buf[k, r, :], b_buf[k, :, pl.ds(at, wide)],
                preferred_element_type=jnp.float32,
            )

    loads_b.wait()
    for h in range(HALVES):
        send_b(has_right, 0, right, gy, h)
        send_b(has_left, 1, left, gy, h)
        send_b(None, 2, across, gy, h)
    for i in range(per):
        loads_a[i].wait()
        for j, g in enumerate(far):
            send_a(1 + j, g, gx * per + i)
    for i in range(per):
        send_a(0, mate, gx * per + i)

    def side(d):
        return ((z - d, z - d >= 0), (z + d, z + d < line))

    def take_line(d, h):
        for way, (s, there) in enumerate(side(d)):
            k = s * 2 + x
            when(there, functools.partial(wait_b, k, h))
            onward, to = (has_right, right) if way == 0 else (has_left, left)
            send_b(both(there, onward), way, to, k, h)
            if d > 1 or h == 1:
                send_b(there, 2, across, k, h)

    def take_left(i):
        for g in far:
            wait_a(g * per + i)
            send_a(0, mate, g * per + i)

    def multiply_line(d):
        @pl.loop(0, 2 * HALVES)
        def _(e):
            w, h = e // HALVES, e % HALVES
            s = z + (2 * w - 1) * d

            @pl.when(jnp.logical_and(s >= 0, s < line))
            def _():
                multiply(s * 2 + x, h)

    def wait_multiply_across(d, h_list):
        for h in h_list:
            @pl.loop(0, 2)
            def _(w):
                s = z + (2 * w - 1) * d

                @pl.when(jnp.logical_and(s >= 0, s < line))
                def _():
                    k = s * 2 + 1 - x
                    wait_b(k, h)
                    multiply(k, h)

    middle = line // 2
    taken_left = 0
    for d in range(1, line):
        for h in range(HALVES):
            take_line(d, h)
        upto = min(per, (per * d + middle - 1) // middle)
        for i in range(taken_left, upto):
            take_left(i)
        taken_left = max(taken_left, upto)
        if d == middle:
            for i in range(taken_left, per):
                take_left(i)
            taken_left = per
            for i in range(per):
                wait_a(mate * per + i)
                for g in far:
                    wait_a((g // 2 * 2 + 1 - g % 2) * per + i)
            load_t.wait()

            @pl.loop(0, HALVES)
            def _(h):
                multiply(gy, h)

            for h in range(HALVES):
                wait_b(across, h)

            @pl.loop(0, HALVES)
            def _(h):
                multiply(across, h)

            for e in range(1, d):
                multiply_line(e)
    send_b(has_right, 0, right, across, 0)
    send_b(has_left, 1, left, across, 0)
    for d in range(middle, line):
        multiply_line(d)
    wait_multiply_across(1, [1])
    for d in range(2, line - 1):
        wait_multiply_across(d, [0, 1])
    wait_multiply_across(1, [0])
    if line - 1 > 1:
        wait_multiply_across(line - 1, [0, 1])

    store = pltpu.make_async_copy(acc, o_hbm, l_sem.at[0])
    store.start()

    @pl.loop(0, rows // LANES)
    def _(i):
        r = pl.ds(pl.multiple_of(i * LANES, LANES), LANES)
        part = jnp.zeros((LANES, LANES), jnp.float32)
        for c in range(cols // LANES):
            v = acc[r, pl.ds(c * LANES, LANES)]
            part += v * v
        p_buf[gx, pl.ds(i, 1), :] = jnp.sum(part.T, axis=0, keepdims=True)

    def p_copy(j, g, slot):
        return pltpu.make_async_remote_copy(
            p_buf.at[slot], p_buf.at[slot], p_send.at[j], p_recv.at[slot],
            device_id=(gy, g), device_id_type=MESH,
        )

    for j, g in enumerate(others):
        p_copy(j, g, gx).start()
    for cond, make in sends:
        when(cond, lambda make=make: make().wait_send())
    for j, g in enumerate(others):
        p_copy(j, g, g).wait_recv()
    total = p_buf[0]
    for g in range(1, m):
        total = total + p_buf[g]
    p_out[...] = total
    for j, g in enumerate(others):
        p_copy(j, g, gx).wait_send()
    store.wait()


def solution(mesh):
    n, m = mesh.shape["gy"], mesh.shape["gx"]

    def on_device(tall_factor, wide_factor, target):
        rows, (depth, cols) = tall_factor.shape[0], wide_factor.shape
        per = tall_factor.shape[1] // depth
        product_sum, row_power = pl.pallas_call(
            functools.partial(kernel, n, m),
            out_shape=(
                jax.ShapeDtypeStruct((rows, cols), jnp.float32),
                jax.ShapeDtypeStruct((rows // LANES, LANES), jnp.float32),
            ),
            in_specs=[pl.BlockSpec(memory_space=pl.ANY)] * 3,
            out_specs=(
                pl.BlockSpec(memory_space=pl.ANY),
                pl.BlockSpec(memory_space=pltpu.VMEM),
            ),
            scratch_shapes=[
                pltpu.VMEM((n, rows, depth), tall_factor.dtype),
                pltpu.VMEM((n, depth, cols), wide_factor.dtype),
                pltpu.VMEM((rows, cols), jnp.float32),
                pltpu.VMEM((m, rows // LANES, LANES), jnp.float32),
                pltpu.SemaphoreType.DMA((n,)),
                pltpu.SemaphoreType.DMA((n, HALVES)),
                pltpu.SemaphoreType.DMA((m,)),
                pltpu.SemaphoreType.DMA((max(2, m // 2), n)),
                pltpu.SemaphoreType.DMA((3, n, HALVES)),
                pltpu.SemaphoreType.DMA((m,)),
                pltpu.SemaphoreType.DMA((2 + per,)),
            ],
            compiler_params=pltpu.CompilerParams(
                collective_id=0, has_side_effects=True, vmem_limit_bytes=56 * 2**20
            ),
        )(tall_factor, wide_factor, target)
        scale = lax.rsqrt(row_power.reshape(rows) / (cols * m) + 1e-06)
        return product_sum * scale[:, None]

    return jax.shard_map(
        on_device,
        mesh=mesh,
        in_specs=(P("gy", "gx"), P("gy", "gx"), P("gy", "gx")),
        out_specs=P("gy", "gx"),
        check_vma=False,
    )
```

```python
import functools

import jax
import jax.numpy as jnp
from jax import lax
from jax.experimental import pallas as pl
from jax.experimental.pallas import tpu as pltpu
from jax.sharding import PartitionSpec as P

MESH = pl.DeviceIdType.MESH
LANES = 128
PARTS = 4


def kernel(
    n, m, a_hbm, b_hbm, t_hbm, acc, p_out,
    a_buf, b_buf, p_buf,
    a_recv, b_recv, p_recv, a_send, b_send, p_send, l_sem,
):
    gy, gx = lax.axis_index("gy"), lax.axis_index("gx")
    depth, cols = b_hbm.shape
    rows = a_hbm.shape[0]
    per = a_hbm.shape[1] // depth
    wide = cols // PARTS
    line = n // 2
    z, x = gy // 2, gy % 2
    has_left, has_right = z > 0, z < line - 1
    left, right, across = gy - 2, gy + 2, z * 2 + 1 - x
    mate = (gx // 2) * 2 + 1 - gx % 2
    others = [lax.rem(gx + j, m) for j in range(1, m)]
    far = [lax.rem(gx + 2 * j, m) for j in range(1, m // 2)]

    loads_b = pltpu.make_async_copy(b_hbm, b_buf.at[gy], l_sem.at[0])
    loads_b.start()
    loads_a = []
    for i in range(per):
        c = pltpu.make_async_copy(
            a_hbm.at[:, pl.ds(i * depth, depth)], a_buf.at[gx * per + i], l_sem.at[2 + i]
        )
        c.start()
        loads_a.append(c)
    load_t = pltpu.make_async_copy(t_hbm, acc, l_sem.at[1])
    load_t.start()

    barrier = pltpu.get_barrier_semaphore()
    for g in others:
        pl.semaphore_signal(barrier, 1, device_id=(gy, g), device_id_type=MESH)
    pl.semaphore_signal(barrier, 1, device_id=(across, gx), device_id_type=MESH)

    @pl.when(has_left)
    def _():
        pl.semaphore_signal(barrier, 1, device_id=(left, gx), device_id_type=MESH)

    @pl.when(has_right)
    def _():
        pl.semaphore_signal(barrier, 1, device_id=(right, gx), device_id_type=MESH)

    pl.semaphore_wait(
        barrier, m + has_left.astype(jnp.int32) + has_right.astype(jnp.int32)
    )

    sends = []

    def when(cond, f):
        if cond is None:
            f()
        else:
            pl.when(cond)(f)

    def both(p, q):
        return q if p is None else jnp.logical_and(p, q)

    def b_copy(way, to, k, h):
        part = b_buf.at[k, :, pl.ds(h * wide, wide)]
        return pltpu.make_async_remote_copy(
            part, part, b_send.at[way, k, h], b_recv.at[k, h],
            device_id=(to, gx), device_id_type=MESH,
        )

    def send_b(cond, way, to, k, h):
        make = functools.partial(b_copy, way, to, k, h)
        when(cond, lambda: make().start())
        sends.append((cond, make))

    def a_copy(way, to, k):
        return pltpu.make_async_remote_copy(
            a_buf.at[k], a_buf.at[k], a_send.at[way, k], a_recv.at[k],
            device_id=(gy, to), device_id_type=MESH,
        )

    def send_a(way, to, k):
        make = functools.partial(a_copy, way, to, k)
        make().start()
        sends.append((None, make))

    def wait_b(k, h):
        b_copy(0, gy, k, h).wait_recv()

    def wait_a(k):
        a_copy(0, gx, k).wait_recv()

    tile = min(rows, 512)

    def multiply(k, h):
        at = pl.multiple_of(h * wide, wide)

        @pl.loop(0, rows // tile)
        def _(i):
            r = pl.ds(pl.multiple_of(i * tile, tile), tile)
            acc[r, pl.ds(at, wide)] -= jnp.dot(
                a_buf[k, r, :], b_buf[k, :, pl.ds(at, wide)],
                preferred_element_type=jnp.float32,
            )

    loads_b.wait()
    for h in range(PARTS):
        send_b(has_right, 0, right, gy, h)
        send_b(has_left, 1, left, gy, h)
        send_b(None, 2, across, gy, h)
    for i in range(per):
        loads_a[i].wait()
        for j, g in enumerate(far):
            send_a(1 + j, g, gx * per + i)
    for i in range(per):
        send_a(0, mate, gx * per + i)

    def side(d):
        return ((z - d, z - d >= 0), (z + d, z + d < line))

    def take_line(d, h):
        for way, (s, there) in enumerate(side(d)):
            k = s * 2 + x
            when(there, functools.partial(wait_b, k, h))
            onward, to = (has_right, right) if way == 0 else (has_left, left)
            send_b(both(there, onward), way, to, k, h)
            if d > 1 or h < PARTS // 2:
                send_b(there, 2, across, k, h)

    def take_left(i):
        for g in far:
            wait_a(g * per + i)
            send_a(0, mate, g * per + i)

    def multiply_line(d, h):
        @pl.loop(0, 2)
        def _(w):
            s = z + (2 * w - 1) * d

            @pl.when(jnp.logical_and(s >= 0, s < line))
            def _():
                multiply(s * 2 + x, h)

    def wait_multiply_across(d, h_list):
        for h in h_list:
            @pl.loop(0, 2)
            def _(w):
                s = z + (2 * w - 1) * d

                @pl.when(jnp.logical_and(s >= 0, s < line))
                def _():
                    k = s * 2 + 1 - x
                    wait_b(k, h)
                    multiply(k, h)

    middle = line // 2
    taken_left = 0
    for d in range(1, line):
        for h in range(PARTS):
            take_line(d, h)
            if d > middle:
                multiply_line(d - 1, h)
                if d == middle + 1 and h < PARTS // 2:
                    wait_multiply_across(1, [h])
        upto = min(per, (per * d + middle - 1) // middle)
        for i in range(taken_left, upto):
            take_left(i)
        taken_left = max(taken_left, upto)
        if d == middle:
            for i in range(taken_left, per):
                take_left(i)
            taken_left = per
            for i in range(per):
                wait_a(mate * per + i)
                for g in far:
                    wait_a((g // 2 * 2 + 1 - g % 2) * per + i)
            load_t.wait()

            @pl.loop(0, PARTS)
            def _(h):
                multiply(gy, h)

            for h in range(PARTS):
                wait_b(across, h)

            @pl.loop(0, PARTS)
            def _(h):
                multiply(across, h)

            for e in range(1, d):
                @pl.loop(0, PARTS)
                def _(h):
                    multiply_line(e, h)

    for h in range(PARTS // 2, PARTS):
        send_b(has_right, 0, right, across, h)
        send_b(has_left, 1, left, across, h)

    @pl.loop(0, PARTS)
    def _(h):
        multiply_line(line - 1, h)

    early, late = list(range(PARTS // 2)), list(range(PARTS // 2, PARTS))
    if line <= middle + 1:
        wait_multiply_across(1, early)
    for d in range(2, line - 1):
        wait_multiply_across(d, early + late)
    wait_multiply_across(1, late)
    if line - 1 > 1:
        wait_multiply_across(line - 1, early + late)

    @pl.loop(0, rows // LANES)
    def _(i):
        r = pl.ds(pl.multiple_of(i * LANES, LANES), LANES)
        part = jnp.zeros((LANES, LANES), jnp.float32)
        for c in range(cols // LANES):
            v = acc[r, pl.ds(c * LANES, LANES)]
            part += v * v
        p_buf[gx, pl.ds(i, 1), :] = jnp.sum(part.T, axis=0, keepdims=True)

    def p_copy(j, g, slot):
        return pltpu.make_async_remote_copy(
            p_buf.at[slot], p_buf.at[slot], p_send.at[j], p_recv.at[slot],
            device_id=(gy, g), device_id_type=MESH,
        )

    for j, g in enumerate(others):
        p_copy(j, g, gx).start()
    for cond, make in sends:
        when(cond, lambda make=make: make().wait_send())
    for j, g in enumerate(others):
        p_copy(j, g, g).wait_recv()
    total = p_buf[0]
    for g in range(1, m):
        total = total + p_buf[g]
    p_out[...] = total
    for j, g in enumerate(others):
        p_copy(j, g, gx).wait_send()


def solution(mesh):
    n, m = mesh.shape["gy"], mesh.shape["gx"]

    def on_device(tall_factor, wide_factor, target):
        rows, (depth, cols) = tall_factor.shape[0], wide_factor.shape
        per = tall_factor.shape[1] // depth
        product_sum, row_power = pl.pallas_call(
            functools.partial(kernel, n, m),
            out_shape=(
                pltpu.VMEM((rows, cols), jnp.float32),
                jax.ShapeDtypeStruct((rows // LANES, LANES), jnp.float32),
            ),
            in_specs=[pl.BlockSpec(memory_space=pltpu.HBM)] * 3,
            out_specs=(
                pl.BlockSpec(memory_space=pltpu.VMEM),
                pl.BlockSpec(memory_space=pltpu.VMEM),
            ),
            scratch_shapes=[
                pltpu.VMEM((n, rows, depth), tall_factor.dtype),
                pltpu.VMEM((n, depth, cols), wide_factor.dtype),
                pltpu.VMEM((m, rows // LANES, LANES), jnp.float32),
                pltpu.SemaphoreType.DMA((n,)),
                pltpu.SemaphoreType.DMA((n, PARTS)),
                pltpu.SemaphoreType.DMA((m,)),
                pltpu.SemaphoreType.DMA((max(2, m // 2), n)),
                pltpu.SemaphoreType.DMA((3, n, PARTS)),
                pltpu.SemaphoreType.DMA((m,)),
                pltpu.SemaphoreType.DMA((2 + per,)),
            ],
            compiler_params=pltpu.CompilerParams(
                collective_id=0, has_side_effects=True, vmem_limit_bytes=67043328 - rows * cols * 4 - 2**17
            ),
        )(tall_factor, wide_factor, target)
        scale = lax.rsqrt(row_power.reshape(rows) / (cols * m) + 1e-06)
        return product_sum * scale[:, None]

    return jax.shard_map(
        on_device,
        mesh=mesh,
        in_specs=(P("gy", "gx"), P("gy", "gx"), P("gy", "gx")),
        out_specs=P("gy", "gx"),
        check_vma=False,
    )
```
